32 devices in a mesh: dp: 8 (over z, y), tp: 4 (over x, core).
Axes of the slice: x: 2, y: 2, z: 4, core: 2. Of those that a mesh axis runs over, the one named last changes fastest.
Arguments:
- queries: bfloat16 [64, 16, 8192], P(('dp', 'tp')), parts along dimension 0, may hold values from -512 to 512
- kv_cache: bfloat16 [64, 8, 384, 256], P(('dp', 'tp')), parts along dimension 0, may hold values from -18 to 18
- lengths: int32 [64], P(('dp', 'tp')), parts along dimension 0, may hold values from 17 to 384, as said below
- residual: bfloat16 [64, 16, 8192], P(('dp', 'tp')), parts along dimension 0, may hold values from -4 to 4
- out_weight: bfloat16 [8192, 8192], P('tp'), may hold values from -0.0625 to 0.0625
- norm_gain: bfloat16 [8192], replicated, may hold values from 0.25 to 1.75
Outputs:
- hidden: bfloat16 [64, 16, 8192], P(('dp', 'tp')), parts along dimension 0
- normed: bfloat16 [64, 16, 8192], P(('dp', 'tp')), parts along dimension 0
The draws below stay inside these ranges and needn't reach their ends.
There are 8 independent parts, one for each index of `dp`. The reference program is written for one: setup_inputs(seed, part) draws one part's arguments, and reference() takes and returns one part's arrays. A program takes and returns all parts, laid end to end along the dimension named above; an argument that names none is the same for every part. Nothing has to cross between parts.
Inputs may be any that keep to these rules, and one draw needn't show every extreme that they name: `lengths`: some sequence of every part has exactly 384 live slots.
All inputs are finite; a program needn't handle non-finite values.
Results may differ from the reference program's by a relative error of at most 0.015.
Values may be sent and summed in bfloat16 or wider, within the bound.
A program may use at most 128 MiB of HBM per device.

```python
import jax
import jax.numpy as jnp
from jax import lax

D = 8192
HEADS = 64
KV_HEADS = 8
HEAD_DIM = 128
DRAFT = 16
LEN = 384
SEQS = 8
N_TP = 4


def draw_queries(key, part):
    normal_part = jnp.clip(jax.random.normal(jax.random.fold_in(key, 11), (SEQS, DRAFT, HEADS * HEAD_DIM), jnp.float32) * 1.5, -9.0, 9.0)
    return normal_part.astype(jnp.bfloat16)


def draw_kv_cache(key, part):
    shape_all = (SEQS, KV_HEADS, LEN, HEAD_DIM)
    key_part = jnp.clip(jax.random.normal(jax.random.fold_in(key, 21), shape_all, jnp.float32), -6.0, 6.0)
    value_part = jnp.clip(jax.random.normal(jax.random.fold_in(key, 22), shape_all, jnp.float32) * 3.0, -18.0, 18.0)
    return jnp.concatenate([key_part, value_part], axis=-1).astype(jnp.bfloat16)


def draw_lengths(key, part):
    drawn = jax.random.randint(jax.random.fold_in(key, 31), (SEQS,), DRAFT + 1, LEN + 1, dtype=jnp.int32)
    return drawn.at[0].set(LEN)


def draw_residual(key, part):
    row_values = jax.random.normal(jax.random.fold_in(key, 41), (SEQS, DRAFT, D), jnp.float32) * 0.5
    return jnp.clip(row_values, -4.0, 4.0).astype(jnp.bfloat16)


def block_scale(own_key, extent, cuts, smallest, top_value):
    loudness, own = 1.0, jax.random.fold_in(own_key, 6)
    for dim, parts in cuts:
        heights = jnp.exp(jax.random.uniform(jax.random.fold_in(own, dim), (parts,), jnp.float32, smallest / len(cuts), top_value / len(cuts)))
        loudness = loudness * jnp.repeat(heights, extent[dim] // parts).reshape([-1 if axis == dim else 1 for axis in range(len(extent))])
    return loudness


def gaussian(key, extent, width, most, shards=(), kind=jnp.bfloat16):
    gain = block_scale(key, extent, shards, -0.22, 0.18) if shards else 1.0
    entries = jax.random.normal(key, extent, jnp.float32) * width * gain
    return jnp.minimum(jnp.maximum(entries, -most), most).astype(kind)


def setup_inputs(seed: int = 0, part: int = 0) -> dict:
    key_list = jax.random.split(jax.random.key(seed), 7)
    own_keys = jax.random.split(jax.random.fold_in(key_list[6], part), 7)
    return {
        "queries": draw_queries(jax.random.fold_in(jax.random.fold_in(key_list[6], part), 71), part),
        "kv_cache": draw_kv_cache(jax.random.fold_in(jax.random.fold_in(key_list[6], part), 71), part),
        "lengths": draw_lengths(jax.random.fold_in(jax.random.fold_in(key_list[6], part), 71), part),
        "residual": draw_residual(jax.random.fold_in(jax.random.fold_in(key_list[6], part), 71), part),
        "out_weight": gaussian(key_list[4], (HEADS * HEAD_DIM, D), (HEADS * HEAD_DIM) ** -0.5, 0.0625, ((0, 4),)),
        "norm_gain": jnp.clip(1.0 + 0.15 * jax.random.normal(key_list[5], (D,), jnp.float32), 0.25, 1.75).astype(jnp.bfloat16),
    }


def attend(queries, kv_cache, lengths):
    seq_count = queries.shape[0]
    per_group = HEADS // KV_HEADS
    grouped = queries.reshape(seq_count, DRAFT, KV_HEADS, per_group, HEAD_DIM).transpose(0, 2, 3, 1, 4)
    grouped = grouped.reshape(seq_count, KV_HEADS, per_group * DRAFT, HEAD_DIM).astype(jnp.float32)
    key_part = kv_cache[..., :HEAD_DIM].astype(jnp.float32)
    value_part = kv_cache[..., HEAD_DIM:].astype(jnp.float32)
    scores = jnp.einsum('skqd,skld->skql', grouped, key_part) * HEAD_DIM ** (-0.5)
    draft_index = jnp.arange(per_group * DRAFT, dtype=jnp.int32) % DRAFT
    visible = lengths[:, None, None, None] - DRAFT + 1 + draft_index[None, None, :, None]
    position = jnp.arange(LEN, dtype=jnp.int32)
    allowed = position[None, None, None, :] < visible
    scores = jnp.where(allowed, scores, -1e+30)
    peak = lax.optimization_barrier(jnp.max(scores, axis=-1, keepdims=True))
    raised = jnp.exp(scores - peak)
    totals = lax.optimization_barrier(jnp.sum(raised, axis=-1, keepdims=True))
    weights = (raised / totals).astype(jnp.bfloat16)
    attended = jnp.einsum('skql,skld->skqd', weights.astype(jnp.float32), value_part).astype(jnp.bfloat16)
    attended = attended.reshape(seq_count, KV_HEADS, per_group, DRAFT, HEAD_DIM).transpose(0, 3, 1, 2, 4)
    return attended.reshape(seq_count, DRAFT, HEADS * HEAD_DIM)

def reference(queries, kv_cache, lengths, residual, out_weight, norm_gain):
    attended = attend(queries, kv_cache, lengths)
    flat_rows = attended.reshape(SEQS * DRAFT, HEADS * HEAD_DIM)
    columns = HEADS * HEAD_DIM // N_TP
    projected = jnp.zeros((SEQS * DRAFT, D), jnp.float32)
    for shard in range(N_TP):
        partial_term = jnp.dot(flat_rows[:, shard * columns:(shard + 1) * columns], out_weight[shard * columns:(shard + 1) * columns], preferred_element_type=jnp.float32)
        projected = projected + lax.optimization_barrier(partial_term.astype(jnp.bfloat16)).astype(jnp.float32)
    summed = residual.astype(jnp.float32) + projected.reshape(SEQS, DRAFT, D)
    hidden = summed.astype(jnp.bfloat16)
    scales = lax.rsqrt(lax.optimization_barrier(jnp.mean(summed * summed, axis=-1, keepdims=True)) + 1e-05)
    normed = (summed * scales * norm_gain.astype(jnp.float32)).astype(jnp.bfloat16)
    return (hidden, normed)
```

```python
import functools
import math

import jax
import jax.numpy as jnp
from jax import lax
from jax.experimental import pallas as pl
from jax.experimental.pallas import tpu as pltpu
from jax.sharding import PartitionSpec as P

CORES = 2
COLUMNS = 512
LANES = 128


def block_kernel(
    n,
    lengths_ref,
    queries_ref,
    kv_ref,
    residual_ref,
    weight_ref,
    gain_ref,
    hidden_ref,
    normed_ref,
    q_buf,
    kv_buf,
    res_buf,
    w_buf,
    gain_buf,
    att_send,
    att,
    keep,
    mate_send,
    mate_recv,
    cross_send,
    cross_recv,
    acc,
    hidden_buf,
    normed_buf,
    load_sem,
    kv_sem,
    w_sem,
    att_send_sem,
    att_recv_sem,
    mate_send_sem,
    mate_recv_sem,
    cross_send_sem,
    cross_recv_sem,
    out_sem,
):
    chips = n // CORES
    seqs, draft, width = queries_ref.shape
    kv_heads, slots_kv, head_dim = kv_ref.shape[1], kv_ref.shape[2], kv_ref.shape[3] // 2
    heads = width // head_dim
    group = heads // kv_heads
    own_heads = heads // n
    unit_heads = min(own_heads, group)
    units = own_heads // unit_heads
    kv_per_dest = kv_buf.shape[2]
    rows = seqs * draft
    chunks, depth, columns = w_buf.shape
    model = chunks * columns

    me = lax.axis_index("tp")
    chip, core = me // CORES, me % CORES

    def device(dx, dk):
        return ((chip + dx) % chips) * CORES + (core + dk) % CORES

    def slot_of(dx, dk):
        return dx * CORES + dk

    order = [(dx, dk) for dx in range(1, chips) for dk in range(CORES)] + [(0, 1), (0, 0)]

    q_copy = pltpu.make_async_copy(queries_ref, q_buf, load_sem.at[0])
    q_copy.start()
    kv_copies = []
    for step, (dx, dk) in enumerate(order):
        first = device(dx, dk) * own_heads // group
        copy = pltpu.make_async_copy(
            kv_ref.at[:, pl.ds(first, kv_per_dest)], kv_buf.at[step], kv_sem.at[step]
        )
        copy.start()
        kv_copies.append(copy)

    def w_copy(c):
        at = pl.multiple_of(c * columns, LANES)
        return pltpu.make_async_copy(
            weight_ref.at[:, pl.ds(at, columns)], w_buf.at[c], w_sem.at[c]
        )

    def start_w(c, carry):
        w_copy(c).start()
        return carry

    lax.fori_loop(0, chunks, start_w, 0)
    res_copy = pltpu.make_async_copy(residual_ref, res_buf, load_sem.at[1])
    res_copy.start()
    gain_copy = pltpu.make_async_copy(gain_ref, gain_buf, load_sem.at[2])
    gain_copy.start()

    barrier = pltpu.get_barrier_semaphore()
    for dx, dk in order[:-1]:
        pl.semaphore_signal(
            barrier,
            inc=1,
            device_id={"tp": device(dx, dk)},
            device_id_type=pl.DeviceIdType.MESH,
        )
    pl.semaphore_wait(barrier, n - 1)

    q_copy.wait()
    position = lax.broadcasted_iota(jnp.int32, (draft, slots_kv), 1)
    token = lax.broadcasted_iota(jnp.int32, (draft, slots_kv), 0)
    biases = [
        jnp.where(position < lengths_ref[s] - draft + 1 + token, 0.0, -1e30).astype(jnp.float32)
        for s in range(seqs)
    ]
    factor = head_dim ** (-0.5) * math.log2(math.e)

    def att_copy(dx, dk, s, source_slot, target_slot):
        part = pl.ds(s * draft, draft)
        return pltpu.make_async_remote_copy(
            src_ref=att_send.at[source_slot, part],
            dst_ref=att.at[target_slot, part],
            send_sem=att_send_sem.at[source_slot, s],
            recv_sem=att_recv_sem.at[target_slot, s],
            device_id={"tp": device(dx, dk)},
            device_id_type=pl.DeviceIdType.MESH,
        )

    for step, (dx, dk) in enumerate(order):
        slot = slot_of(dx, dk)
        dest = device(dx, dk)
        kv_copies[step].wait()
        target = att if slot == 0 else att_send
        for s in range(seqs):
            for u in range(units):
                kv_at = u if own_heads >= group else 0
                start = pl.multiple_of((dest * own_heads + u * unit_heads) * head_dim, LANES)
                wide = q_buf[s, :, pl.ds(start, unit_heads * head_dim)]
                q_rows = jnp.concatenate(
                    [wide[:, h * head_dim : (h + 1) * head_dim] for h in range(unit_heads)], axis=0
                )
                keys = kv_buf[step, s, kv_at, :, :head_dim]
                values = kv_buf[step, s, kv_at, :, head_dim:]
                scores = lax.dot_general(
                    q_rows, keys, (((1,), (1,)), ((), ())), preferred_element_type=jnp.float32
                )
                scores = scores.reshape(unit_heads, draft, slots_kv) + biases[s][None]
                peak = jnp.max(scores, axis=-1, keepdims=True)
                raised = jnp.exp2((scores - peak) * factor)
                totals = jnp.sum(raised, axis=-1, keepdims=True)
                out = jnp.dot(
                    raised.astype(jnp.bfloat16).reshape(unit_heads * draft, slots_kv),
                    values,
                    preferred_element_type=jnp.float32,
                )
                out = (out * (1.0 / totals).reshape(unit_heads * draft, 1)).astype(jnp.bfloat16)
                for h in range(unit_heads):
                    at = (u * unit_heads + h) * head_dim
                    target[slot, s * draft : (s + 1) * draft, at : at + head_dim] = out[
                        h * draft : (h + 1) * draft
                    ]
            if slot:
                att_copy(dx, dk, s, slot, slot_of((chips - dx) % chips, dk)).start()

    for dx, dk in order[:-1]:
        slot = slot_of(dx, dk)
        for s in range(seqs):
            att_copy(dx, dk, s, slot, slot).wait_recv()

    def mate_copy(c):
        return pltpu.make_async_remote_copy(
            src_ref=mate_send.at[c],
            dst_ref=mate_recv.at[c],
            send_sem=mate_send_sem.at[c],
            recv_sem=mate_recv_sem.at[c],
            device_id={"tp": device(0, 1)},
            device_id_type=pl.DeviceIdType.MESH,
        )

    def cross_copy(dx, source, target, c):
        return pltpu.make_async_remote_copy(
            src_ref=cross_send.at[source, c],
            dst_ref=cross_recv.at[target, c],
            send_sem=cross_send_sem.at[source, c],
            recv_sem=cross_recv_sem.at[target, c],
            device_id={"tp": device(dx, 0)},
            device_id_type=pl.DeviceIdType.MESH,
        )

    def multiply(c):
        w_copy(c).wait()
        product = jnp.dot(
            att[...].reshape(n * rows, depth), w_buf[c], preferred_element_type=jnp.float32
        )
        for dx in range(chips):
            own, other = slot_of(dx, 0) * rows, slot_of(dx, 1) * rows
            mate_send[c, dx] = product[other : other + rows].astype(jnp.bfloat16)
            keep[c % 2, dx] = product[own : own + rows]
        mate_copy(c).start()

    def pass_on(c):
        mate_copy(c).wait_recv()
        for dx in range(1, chips):
            both = keep[c % 2, dx] + mate_recv[c, dx].astype(jnp.float32)
            cross_send[dx - 1, c] = both.astype(jnp.bfloat16)
            cross_copy(dx, dx - 1, chips - dx - 1, c).start()
        acc[c] = keep[c % 2, 0] + mate_recv[c, 0].astype(jnp.float32)

    multiply(0)

    def both_steps(c, carry):
        multiply(c)
        pass_on(c - 1)
        return carry

    lax.fori_loop(1, chunks, both_steps, 0)
    pass_on(chunks - 1)

    res_copy.wait()

    def collect(c, squares):
        at = pl.multiple_of(c * columns, LANES)
        total = acc[c]
        for dx in range(1, chips):
            cross_copy(dx, dx - 1, dx - 1, c).wait_recv()
            total = total + cross_recv[dx - 1, c].astype(jnp.float32)
        total = total + res_buf[:, :, pl.ds(at, columns)].astype(jnp.float32).reshape(rows, columns)
        acc[c] = total
        hidden_buf[:, :, pl.ds(at, columns)] = total.astype(jnp.bfloat16).reshape(
            seqs, draft, columns
        )
        for tile in range(columns // LANES):
            part = total[:, tile * LANES : (tile + 1) * LANES]
            squares = squares + part * part
        return squares

    squares = lax.fori_loop(0, chunks, collect, jnp.zeros((rows, LANES), jnp.float32))
    hidden_copy = pltpu.make_async_copy(hidden_buf, hidden_ref, out_sem.at[0])
    hidden_copy.start()
    scales = lax.rsqrt(jnp.sum(squares, axis=-1, keepdims=True) / model + 1e-05)
    gain_copy.wait()

    def normalize(c, carry):
        at = pl.multiple_of(c * columns, LANES)
        gain = gain_buf[:, pl.ds(at, columns)].astype(jnp.float32)
        normed = (acc[c] * scales * gain).astype(jnp.bfloat16)
        normed_buf[:, :, pl.ds(at, columns)] = normed.reshape(seqs, draft, columns)
        return carry

    lax.fori_loop(0, chunks, normalize, 0)
    normed_copy = pltpu.make_async_copy(normed_buf, normed_ref, out_sem.at[1])
    normed_copy.start()

    for dx, dk in order[:-1]:
        slot = slot_of(dx, dk)
        for s in range(seqs):
            att_copy(dx, dk, s, slot, slot).wait_send()

    def settle(c, carry):
        mate_copy(c).wait_send()
        for dx in range(1, chips):
            cross_copy(dx, dx - 1, dx - 1, c).wait_send()
        return carry

    lax.fori_loop(0, chunks, settle, 0)
    hidden_copy.wait()
    normed_copy.wait()


def on_device(n, queries, kv_cache, lengths, residual, out_weight, norm_gain):
    seqs, draft, width = queries.shape
    kv_heads, slots_kv, pair_dim = kv_cache.shape[1:]
    head_dim = pair_dim // 2
    heads = width // head_dim
    depth, model = out_weight.shape
    chips = n // CORES
    rows = seqs * draft
    columns = math.gcd(model, COLUMNS)
    chunks = model // columns
    kv_per_dest = max(1, kv_heads // n)
    bf16, f32 = jnp.bfloat16, jnp.float32
    dma = pltpu.SemaphoreType.DMA
    out = jax.ShapeDtypeStruct(residual.shape, bf16)
    return pl.pallas_call(
        functools.partial(block_kernel, n),
        out_shape=(out, out),
        in_specs=[pl.BlockSpec(memory_space=pltpu.SMEM)]
        + [pl.BlockSpec(memory_space=pl.ANY)] * 5,
        out_specs=[pl.BlockSpec(memory_space=pl.ANY)] * 2,
        scratch_shapes=[
            pltpu.VMEM(queries.shape, bf16),
            pltpu.VMEM((n, seqs, kv_per_dest, slots_kv, pair_dim), bf16),
            pltpu.VMEM(residual.shape, bf16),
            pltpu.VMEM((chunks, depth, columns), bf16),
            pltpu.VMEM((1, model), bf16),
            pltpu.VMEM((n, rows, depth), bf16),
            pltpu.VMEM((n, rows, depth), bf16),
            pltpu.VMEM((2, chips, rows, columns), f32),
            pltpu.VMEM((chunks, chips, rows, columns), bf16),
            pltpu.VMEM((chunks, chips, rows, columns), bf16),
            pltpu.VMEM((max(1, chips - 1), chunks, rows, columns), bf16),
            pltpu.VMEM((max(1, chips - 1), chunks, rows, columns), bf16),
            pltpu.VMEM((chunks, rows, columns), f32),
            pltpu.VMEM(residual.shape, bf16),
            pltpu.VMEM(residual.shape, bf16),
            dma((3,)),
            dma((n,)),
            dma((chunks,)),
            dma((n, seqs)),
            dma((n, seqs)),
            dma((chunks,)),
            dma((chunks,)),
            dma((max(1, chips - 1), chunks)),
            dma((max(1, chips - 1), chunks)),
            dma((2,)),
        ],
        compiler_params=pltpu.CompilerParams(
            collective_id=0, has_side_effects=True, vmem_limit_bytes=60 * 1024 * 1024
        ),
    )(lengths, queries, kv_cache, residual, out_weight, norm_gain.reshape(1, model))


def solution(mesh):
    return jax.shard_map(
        functools.partial(on_device, mesh.shape["tp"]),
        mesh=mesh,
        in_specs=(
            P(("dp", "tp"), None, None),
            P(("dp", "tp"), None, None, None),
            P(("dp", "tp")),
            P(("dp", "tp"), None, None),
            P("tp", None),
            P(),
        ),
        out_specs=(P(("dp", "tp"), None, None), P(("dp", "tp"), None, None)),
        check_vma=False,
    )
```

```python
import functools
import math

import jax
import jax.numpy as jnp
from jax import lax
from jax.experimental import pallas as pl
from jax.experimental.pallas import tpu as pltpu
from jax.sharding import PartitionSpec as P

CORES = 2
COLUMNS = 512
LANES = 128


def block_kernel(
    n,
    lengths_ref,
    queries_ref,
    kv_ref,
    residual_ref,
    weight_ref,
    acc,
    scaled_ref,
    q_buf,
    kv_buf,
    res_buf,
    w_buf,
    att_send,
    att,
    keep,
    mate_send,
    mate_recv,
    cross_send,
    cross_recv,
    load_sem,
    kv_sem,
    w_sem,
    att_send_sem,
    att_recv_sem,
    mate_send_sem,
    mate_recv_sem,
    cross_send_sem,
    cross_recv_sem,
):
    chips = n // CORES
    seqs, draft, width = queries_ref.shape
    kv_heads, slots_kv, head_dim = kv_ref.shape[1], kv_ref.shape[2], kv_ref.shape[3] // 2
    heads = width // head_dim
    group = heads // kv_heads
    own_heads = heads // n
    unit_heads = min(own_heads, group)
    units = own_heads // unit_heads
    kv_per_dest = kv_buf.shape[2]
    rows = seqs * draft
    chunks, depth, columns = w_buf.shape
    model = chunks * columns

    me = lax.axis_index("tp")
    chip, core = me // CORES, me % CORES

    def device(dx, dk):
        return ((chip + dx) % chips) * CORES + (core + dk) % CORES

    def slot_of(dx, dk):
        return dx * CORES + dk

    order = [(dx, dk) for dx in range(1, chips) for dk in range(CORES)] + [(0, 1), (0, 0)]

    q_copy = pltpu.make_async_copy(queries_ref, q_buf, load_sem.at[0])
    q_copy.start()
    kv_copies = []
    for step, (dx, dk) in enumerate(order):
        first = device(dx, dk) * own_heads // group
        copy = pltpu.make_async_copy(
            kv_ref.at[:, pl.ds(first, kv_per_dest)], kv_buf.at[step], kv_sem.at[step]
        )
        copy.start()
        kv_copies.append(copy)

    def w_copy(c):
        at = pl.multiple_of(c * columns, LANES)
        return pltpu.make_async_copy(
            weight_ref.at[:, pl.ds(at, columns)], w_buf.at[c], w_sem.at[c]
        )

    def start_w(c, carry):
        w_copy(c).start()
        return carry

    lax.fori_loop(0, chunks, start_w, 0)
    res_copy = pltpu.make_async_copy(residual_ref, res_buf, load_sem.at[1])
    res_copy.start()

    barrier = pltpu.get_barrier_semaphore()
    for dx, dk in order[:-1]:
        pl.semaphore_signal(
            barrier,
            inc=1,
            device_id={"tp": device(dx, dk)},
            device_id_type=pl.DeviceIdType.MESH,
        )
    pl.semaphore_wait(barrier, n - 1)

    q_copy.wait()
    position = lax.broadcasted_iota(jnp.int32, (draft, slots_kv), 1)
    token = lax.broadcasted_iota(jnp.int32, (draft, slots_kv), 0)
    biases = [
        jnp.where(position < lengths_ref[s] - draft + 1 + token, 0.0, -1e30).astype(jnp.float32)
        for s in range(seqs)
    ]
    factor = head_dim ** (-0.5) * math.log2(math.e)

    def att_copy(dx, dk, s, source_slot, target_slot):
        part = pl.ds(s * draft, draft)
        return pltpu.make_async_remote_copy(
            src_ref=att_send.at[source_slot, part],
            dst_ref=att.at[target_slot, part],
            send_sem=att_send_sem.at[source_slot, s],
            recv_sem=att_recv_sem.at[target_slot, s],
            device_id={"tp": device(dx, dk)},
            device_id_type=pl.DeviceIdType.MESH,
        )

    for step, (dx, dk) in enumerate(order):
        slot = slot_of(dx, dk)
        dest = device(dx, dk)
        kv_copies[step].wait()
        target = att if slot == 0 else att_send
        for s in range(seqs):
            for u in range(units):
                kv_at = u if own_heads >= group else 0
                start = pl.multiple_of((dest * own_heads + u * unit_heads) * head_dim, LANES)
                wide = q_buf[s, :, pl.ds(start, unit_heads * head_dim)]
                q_rows = jnp.concatenate(
                    [wide[:, h * head_dim : (h + 1) * head_dim] for h in range(unit_heads)], axis=0
                )
                keys = kv_buf[step, s, kv_at, :, :head_dim]
                values = kv_buf[step, s, kv_at, :, head_dim:]
                scores = lax.dot_general(
                    q_rows, keys, (((1,), (1,)), ((), ())), preferred_element_type=jnp.float32
                )
                scores = scores.reshape(unit_heads, draft, slots_kv) + biases[s][None]
                peak = jnp.max(scores, axis=-1, keepdims=True)
                raised = jnp.exp2((scores - peak) * factor)
                totals = jnp.sum(raised, axis=-1, keepdims=True)
                out = jnp.dot(
                    raised.astype(jnp.bfloat16).reshape(unit_heads * draft, slots_kv),
                    values,
                    preferred_element_type=jnp.float32,
                )
                out = (out * (1.0 / totals).reshape(unit_heads * draft, 1)).astype(jnp.bfloat16)
                for h in range(unit_heads):
                    at = (u * unit_heads + h) * head_dim
                    target[slot, s * draft : (s + 1) * draft, at : at + head_dim] = out[
                        h * draft : (h + 1) * draft
                    ]
            if slot:
                att_copy(dx, dk, s, slot, slot_of((chips - dx) % chips, dk)).start()

    for dx, dk in order[:-1]:
        slot = slot_of(dx, dk)
        for s in range(seqs):
            att_copy(dx, dk, s, slot, slot).wait_recv()

    def mate_copy(c):
        return pltpu.make_async_remote_copy(
            src_ref=mate_send.at[c],
            dst_ref=mate_recv.at[c],
            send_sem=mate_send_sem.at[c],
            recv_sem=mate_recv_sem.at[c],
            device_id={"tp": device(0, 1)},
            device_id_type=pl.DeviceIdType.MESH,
        )

    def cross_copy(dx, source, target, c):
        return pltpu.make_async_remote_copy(
            src_ref=cross_send.at[source, c],
            dst_ref=cross_recv.at[target, c],
            send_sem=cross_send_sem.at[source, c],
            recv_sem=cross_recv_sem.at[target, c],
            device_id={"tp": device(dx, 0)},
            device_id_type=pl.DeviceIdType.MESH,
        )

    def multiply(c):
        w_copy(c).wait()
        product = jnp.dot(
            att[...].reshape(n * rows, depth), w_buf[c], preferred_element_type=jnp.float32
        )
        for dx in range(chips):
            own, other = slot_of(dx, 0) * rows, slot_of(dx, 1) * rows
            mate_send[c, dx] = product[other : other + rows].astype(jnp.bfloat16)
            keep[c % 2, dx] = product[own : own + rows]
        mate_copy(c).start()

    def pass_on(c):
        mate_copy(c).wait_recv()
        for dx in range(1, chips):
            both = keep[c % 2, dx] + mate_recv[c, dx].astype(jnp.float32)
            cross_send[dx - 1, c] = both.astype(jnp.bfloat16)
            cross_copy(dx, dx - 1, chips - dx - 1, c).start()
        at = pl.multiple_of(c * columns, LANES)
        own = keep[c % 2, 0] + mate_recv[c, 0].astype(jnp.float32)
        acc[:, :, pl.ds(at, columns)] = own.reshape(seqs, draft, columns)

    multiply(0)

    def both_steps(c, carry):
        multiply(c)
        pass_on(c - 1)
        return carry

    lax.fori_loop(1, chunks, both_steps, 0)
    pass_on(chunks - 1)

    res_copy.wait()

    def collect(c, squares):
        at = pl.multiple_of(c * columns, LANES)
        total = acc[:, :, pl.ds(at, columns)]
        for dx in range(1, chips):
            cross_copy(dx, dx - 1, dx - 1, c).wait_recv()
            part = cross_recv[dx - 1, c].astype(jnp.float32)
            total = total + part.reshape(seqs, draft, columns)
        total = total + res_buf[:, :, pl.ds(at, columns)].astype(jnp.float32)
        acc[:, :, pl.ds(at, columns)] = total
        for tile in range(columns // LANES):
            part = total[:, :, tile * LANES : (tile + 1) * LANES]
            squares = squares + part * part
        return squares

    squares = lax.fori_loop(0, chunks, collect, jnp.zeros((seqs, draft, LANES), jnp.float32))
    scales = lax.rsqrt(jnp.sum(squares, axis=-1, keepdims=True) / model + 1e-05)

    def scale(c, carry):
        at = pl.multiple_of(c * columns, LANES)
        scaled_ref[:, :, pl.ds(at, columns)] = acc[:, :, pl.ds(at, columns)] * scales
        return carry

    lax.fori_loop(0, chunks, scale, 0)

    for dx, dk in order[:-1]:
        slot = slot_of(dx, dk)
        for s in range(seqs):
            att_copy(dx, dk, s, slot, slot).wait_send()

    def settle(c, carry):
        mate_copy(c).wait_send()
        for dx in range(1, chips):
            cross_copy(dx, dx - 1, dx - 1, c).wait_send()
        return carry

    lax.fori_loop(0, chunks, settle, 0)


def on_device(n, queries, kv_cache, lengths, residual, out_weight, norm_gain):
    seqs, draft, width = queries.shape
    kv_heads, slots_kv, pair_dim = kv_cache.shape[1:]
    head_dim = pair_dim // 2
    heads = width // head_dim
    depth, model = out_weight.shape
    chips = n // CORES
    rows = seqs * draft
    columns = math.gcd(model, COLUMNS)
    chunks = model // columns
    kv_per_dest = max(1, kv_heads // n)
    bf16, f32 = jnp.bfloat16, jnp.float32
    dma = pltpu.SemaphoreType.DMA
    summed, scaled = pl.pallas_call(
        functools.partial(block_kernel, n),
        out_shape=(
            pltpu.VMEM(residual.shape, f32),
            pltpu.VMEM(residual.shape, f32),
        ),
        in_specs=[pl.BlockSpec(memory_space=pltpu.SMEM)]
        + [pl.BlockSpec(memory_space=pl.ANY)] * 4,
        out_specs=[pl.BlockSpec(memory_space=pltpu.VMEM)] * 2,
        scratch_shapes=[
            pltpu.VMEM(queries.shape, bf16),
            pltpu.VMEM((n, seqs, kv_per_dest, slots_kv, pair_dim), bf16),
            pltpu.VMEM(residual.shape, bf16),
            pltpu.VMEM((chunks, depth, columns), bf16),
            pltpu.VMEM((n, rows, depth), bf16),
            pltpu.VMEM((n, rows, depth), bf16),
            pltpu.VMEM((2, chips, rows, columns), f32),
            pltpu.VMEM((chunks, chips, rows, columns), bf16),
            pltpu.VMEM((chunks, chips, rows, columns), bf16),
            pltpu.VMEM((max(1, chips - 1), chunks, rows, columns), bf16),
            pltpu.VMEM((max(1, chips - 1), chunks, rows, columns), bf16),
            dma((2,)),
            dma((n,)),
            dma((chunks,)),
            dma((n, seqs)),
            dma((n, seqs)),
            dma((chunks,)),
            dma((chunks,)),
            dma((max(1, chips - 1), chunks)),
            dma((max(1, chips - 1), chunks)),
        ],
        compiler_params=pltpu.CompilerParams(
            collective_id=0, has_side_effects=True, vmem_limit_bytes=56 * 1024 * 1024
        ),
    )(lengths, queries, kv_cache, residual, out_weight)
    normed = scaled * norm_gain.astype(f32)
    return summed.astype(bf16), normed.astype(bf16)


def solution(mesh):
    return jax.shard_map(
        functools.partial(on_device, mesh.shape["tp"]),
        mesh=mesh,
        in_specs=(
            P(("dp", "tp"), None, None),
            P(("dp", "tp"), None, None, None),
            P(("dp", "tp")),
            P(("dp", "tp"), None, None),
            P("tp", None),
            P(),
        ),
        out_specs=(P(("dp", "tp"), None, None), P(("dp", "tp"), None, None)),
        check_vma=False,
    )
```

```python
import functools
import math

import jax
import jax.numpy as jnp
from jax import lax
from jax.experimental import pallas as pl
from jax.experimental.pallas import tpu as pltpu
from jax.sharding import PartitionSpec as P

CORES = 2
COLUMNS = 512
LANES = 128
LAG = 4
EARLY = 8


def block_kernel(
    n,
    lengths_ref,
    queries_ref,
    kv_ref,
    residual_ref,
    weight_ref,
    acc,
    scaled_ref,
    q_buf,
    kv_buf,
    res_buf,
    w_buf,
    att_send,
    att,
    keep,
    mate_send,
    mate_recv,
    early_send,
    early_recv,
    cross_send,
    cross_recv,
    load_sem,
    kv_sem,
    w_sem,
    att_send_sem,
    att_recv_sem,
    mate_send_sem,
    mate_recv_sem,
    early_send_sem,
    early_recv_sem,
    cross_send_sem,
    cross_recv_sem,
):
    chips = n // CORES
    seqs, draft, width = queries_ref.shape
    kv_heads, slots_kv, head_dim = kv_ref.shape[1], kv_ref.shape[2], kv_ref.shape[3] // 2
    heads = width // head_dim
    group = heads // kv_heads
    own_heads = heads // n
    unit_heads = min(own_heads, group)
    units = own_heads // unit_heads
    kv_per_dest = kv_buf.shape[2]
    rows = seqs * draft
    chunks, depth, columns = w_buf.shape
    model = chunks * columns
    half = cross_send.shape[3]
    halves = rows // half
    half_seqs = half // draft
    early = early_send.shape[0] if halves > 1 and chips > 1 else 0
    ring = keep.shape[0]
    lag = ring - 1

    me = lax.axis_index("tp")
    chip, core = me // CORES, me % CORES

    def device(dx, dk):
        return ((chip + dx) % chips) * CORES + (core + dk) % CORES

    def slot_of(dx, dk):
        return dx * CORES + dk

    order = [(dx, dk) for dx in range(1, chips) for dk in range(CORES)] + [(0, 1), (0, 0)]

    q_copy = pltpu.make_async_copy(queries_ref, q_buf, load_sem.at[0])
    q_copy.start()
    kv_copies = []
    for step, (dx, dk) in enumerate(order):
        first = device(dx, dk) * own_heads // group
        copy = pltpu.make_async_copy(
            kv_ref.at[:, pl.ds(first, kv_per_dest)], kv_buf.at[step], kv_sem.at[step]
        )
        copy.start()
        kv_copies.append(copy)

    def w_copy(c):
        at = pl.multiple_of(c * columns, LANES)
        return pltpu.make_async_copy(
            weight_ref.at[:, pl.ds(at, columns)], w_buf.at[c], w_sem.at[c]
        )

    def start_w(c, carry):
        w_copy(c).start()
        return carry

    lax.fori_loop(0, chunks, start_w, 0)
    res_copy = pltpu.make_async_copy(residual_ref, res_buf, load_sem.at[1])
    res_copy.start()

    barrier = pltpu.get_barrier_semaphore()
    for dx, dk in order[:-1]:
        pl.semaphore_signal(
            barrier,
            inc=1,
            device_id={"tp": device(dx, dk)},
            device_id_type=pl.DeviceIdType.MESH,
        )
    pl.semaphore_wait(barrier, n - 1)

    q_copy.wait()
    position = lax.broadcasted_iota(jnp.int32, (draft, slots_kv), 1)
    token = lax.broadcasted_iota(jnp.int32, (draft, slots_kv), 0)
    biases = [
        jnp.where(position < lengths_ref[s] - draft + 1 + token, 0.0, -1e30).astype(jnp.float32)
        for s in range(seqs)
    ]
    factor = head_dim ** (-0.5) * math.log2(math.e)

    def att_copy(dx, dk, s, source_slot, target_slot):
        part = pl.ds(s * draft, draft)
        return pltpu.make_async_remote_copy(
            src_ref=att_send.at[source_slot, part],
            dst_ref=att.at[target_slot, part],
            send_sem=att_send_sem.at[source_slot, s],
            recv_sem=att_recv_sem.at[target_slot, s],
            device_id={"tp": device(dx, dk)},
            device_id_type=pl.DeviceIdType.MESH,
        )

    cross_steps = list(range(len(order) - CORES))
    near_steps = list(range(len(order) - CORES, len(order)))
    todo = [(step, s) for s in range(seqs) for step in cross_steps]
    todo += [(step, s) for step in near_steps for s in range(seqs)]
    loaded = set()
    for step, s in todo:
        dx, dk = order[step]
        slot = slot_of(dx, dk)
        dest = device(dx, dk)
        if step not in loaded:
            kv_copies[step].wait()
            loaded.add(step)
        target = att if slot == 0 else att_send
        for u in range(units):
            kv_at = u if own_heads >= group else 0
            start = pl.multiple_of((dest * own_heads + u * unit_heads) * head_dim, LANES)
            wide = q_buf[s, :, pl.ds(start, unit_heads * head_dim)]
            q_rows = jnp.concatenate(
                [wide[:, h * head_dim : (h + 1) * head_dim] for h in range(unit_heads)], axis=0
            )
            keys = kv_buf[step, s, kv_at, :, :head_dim]
            values = kv_buf[step, s, kv_at, :, head_dim:]
            scores = lax.dot_general(
                q_rows, keys, (((1,), (1,)), ((), ())), preferred_element_type=jnp.float32
            )
            scores = scores.reshape(unit_heads, draft, slots_kv) + biases[s][None]
            peak = jnp.max(scores, axis=-1, keepdims=True)
            raised = jnp.exp2((scores - peak) * factor)
            totals = jnp.sum(raised, axis=-1, keepdims=True)
            out = jnp.dot(
                raised.astype(jnp.bfloat16).reshape(unit_heads * draft, slots_kv),
                values,
                preferred_element_type=jnp.float32,
            )
            out = (out * (1.0 / totals).reshape(unit_heads * draft, 1)).astype(jnp.bfloat16)
            for h in range(unit_heads):
                at = (u * unit_heads + h) * head_dim
                target[slot, s * draft : (s + 1) * draft, at : at + head_dim] = out[
                    h * draft : (h + 1) * draft
                ]
        if slot:
            att_copy(dx, dk, s, slot, slot_of((chips - dx) % chips, dk)).start()

    def arrived(step, s):
        dx, dk = order[step]
        slot = slot_of(dx, dk)
        att_copy(dx, dk, s, slot, slot).wait_recv()

    def to_mate(source, target, send_sem, recv_sem, c):
        return pltpu.make_async_remote_copy(
            src_ref=source.at[c],
            dst_ref=target.at[c],
            send_sem=send_sem.at[c],
            recv_sem=recv_sem.at[c],
            device_id={"tp": device(0, 1)},
            device_id_type=pl.DeviceIdType.MESH,
        )

    mate_copy = functools.partial(to_mate, mate_send, mate_recv, mate_send_sem, mate_recv_sem)
    early_copy = functools.partial(to_mate, early_send, early_recv, early_send_sem, early_recv_sem)

    def cross_copy(dx, source, target, c, h):
        return pltpu.make_async_remote_copy(
            src_ref=cross_send.at[source, c, h],
            dst_ref=cross_recv.at[target, c, h],
            send_sem=cross_send_sem.at[source, c, h],
            recv_sem=cross_recv_sem.at[target, c, h],
            device_id={"tp": device(dx, 0)},
            device_id_type=pl.DeviceIdType.MESH,
        )

    def send_sum(dx, c, h, mine, mates):
        cross_send[dx - 1, c, h] = (mine + mates.astype(jnp.float32)).astype(jnp.bfloat16)
        cross_copy(dx, dx - 1, chips - dx - 1, c, h).start()

    if early:
        for s in range(half_seqs):
            for step in cross_steps:
                arrived(step, s)

        def early_multiply(c):
            w_copy(c).wait()
            first = att[CORES:, :half].reshape((n - CORES) * half, depth)
            product = jnp.dot(first, w_buf[c], preferred_element_type=jnp.float32)
            for dx in range(1, chips):
                own = (slot_of(dx, 0) - CORES) * half
                other = (slot_of(dx, 1) - CORES) * half
                early_send[c, dx - 1] = product[other : other + half].astype(jnp.bfloat16)
                keep[c % ring, dx, :half] = product[own : own + half]
            early_copy(c).start()

        def early_pass(c):
            early_copy(c).wait_recv()
            for dx in range(1, chips):
                send_sum(dx, c, 0, keep[c % ring, dx, :half], early_recv[c, dx - 1])

        def early_step(c, carry):
            @pl.when(c < early)
            def _():
                early_multiply(c)

            @pl.when(c >= lag)
            def _():
                early_pass(c - lag)

            return carry

        lax.fori_loop(0, early + lag, early_step, 0)

    for s in range(half_seqs if early else 0, seqs):
        for step in cross_steps:
            arrived(step, s)
    for s in range(seqs):
        arrived(near_steps[0], s)

    def multiply(c):
        @pl.when(c >= early)
        def _():
            w_copy(c).wait()

        product = jnp.dot(
            att[...].reshape(n * rows, depth), w_buf[c], preferred_element_type=jnp.float32
        )
        for dx in range(chips):
            own, other = slot_of(dx, 0) * rows, slot_of(dx, 1) * rows
            mate_send[c, dx] = product[other : other + rows].astype(jnp.bfloat16)
            keep[c % ring, dx] = product[own : own + rows]
        mate_copy(c).start()

    def pass_on(c):
        mate_copy(c).wait_recv()
        for dx in range(1, chips):
            for h in range(halves):
                part = pl.ds(h * half, half)

                def send():
                    send_sum(dx, c, h, keep[c % ring, dx, part], mate_recv[c, dx, part])

                if h == 0 and early:
                    pl.when(c >= early)(send)
                else:
                    send()
        at = pl.multiple_of(c * columns, LANES)
        own = keep[c % ring, 0] + mate_recv[c, 0].astype(jnp.float32)
        acc[:, :, pl.ds(at, columns)] = own.reshape(seqs, draft, columns)

    def both_steps(c, carry):
        @pl.when(c < chunks)
        def _():
            multiply(c)

        @pl.when(c >= lag)
        def _():
            pass_on(c - lag)

        return carry

    lax.fori_loop(0, chunks + lag, both_steps, 0)

    res_copy.wait()

    def collect(c, squares):
        at = pl.multiple_of(c * columns, LANES)
        total = acc[:, :, pl.ds(at, columns)]
        for dx in range(1, chips):
            for h in range(halves):
                cross_copy(dx, dx - 1, dx - 1, c, h).wait_recv()
            part = cross_recv[dx - 1, c].astype(jnp.float32)
            total = total + part.reshape(seqs, draft, columns)
        total = total + res_buf[:, :, pl.ds(at, columns)].astype(jnp.float32)
        acc[:, :, pl.ds(at, columns)] = total
        for tile in range(columns // LANES):
            part = total[:, :, tile * LANES : (tile + 1) * LANES]
            squares = squares + part * part
        return squares

    squares = lax.fori_loop(0, chunks, collect, jnp.zeros((seqs, draft, LANES), jnp.float32))
    scales = lax.rsqrt(jnp.sum(squares, axis=-1, keepdims=True) / model + 1e-05)

    def scale(c, carry):
        at = pl.multiple_of(c * columns, LANES)
        scaled_ref[:, :, pl.ds(at, columns)] = acc[:, :, pl.ds(at, columns)] * scales
        return carry

    lax.fori_loop(0, chunks, scale, 0)

    for dx, dk in order[:-1]:
        slot = slot_of(dx, dk)
        for s in range(seqs):
            att_copy(dx, dk, s, slot, slot).wait_send()

    def settle(c, carry):
        mate_copy(c).wait_send()
        for dx in range(1, chips):
            for h in range(halves):
                cross_copy(dx, dx - 1, dx - 1, c, h).wait_send()
        return carry

    lax.fori_loop(0, chunks, settle, 0)
    for c in range(early):
        early_copy(c).wait_send()


def on_device(n, queries, kv_cache, lengths, residual, out_weight, norm_gain):
    seqs, draft, width = queries.shape
    kv_heads, slots_kv, pair_dim = kv_cache.shape[1:]
    head_dim = pair_dim // 2
    heads = width // head_dim
    depth, model = out_weight.shape
    chips = n // CORES
    rows = seqs * draft
    columns = math.gcd(model, COLUMNS)
    chunks = model // columns
    kv_per_dest = max(1, kv_heads // n)
    half = rows // 2 if seqs % 2 == 0 else rows
    halves = rows // half
    early = min(EARLY, chunks)
    others = max(1, chips - 1)
    bf16, f32 = jnp.bfloat16, jnp.float32
    dma = pltpu.SemaphoreType.DMA
    summed, scaled = pl.pallas_call(
        functools.partial(block_kernel, n),
        out_shape=(
            pltpu.VMEM(residual.shape, f32),
            pltpu.VMEM(residual.shape, f32),
        ),
        in_specs=[pl.BlockSpec(memory_space=pltpu.SMEM)]
        + [pl.BlockSpec(memory_space=pl.ANY)] * 4,
        out_specs=[pl.BlockSpec(memory_space=pltpu.VMEM)] * 2,
        scratch_shapes=[
            pltpu.VMEM(queries.shape, bf16),
            pltpu.VMEM((n, seqs, kv_per_dest, slots_kv, pair_dim), bf16),
            pltpu.VMEM(residual.shape, bf16),
            pltpu.VMEM((chunks, depth, columns), bf16),
            pltpu.VMEM((n, rows, depth), bf16),
            pltpu.VMEM((n, rows, depth), bf16),
            pltpu.VMEM((LAG + 1, chips, rows, columns), f32),
            pltpu.VMEM((chunks, chips, rows, columns), bf16),
            pltpu.VMEM((chunks, chips, rows, columns), bf16),
            pltpu.VMEM((early, others, half, columns), bf16),
            pltpu.VMEM((early, others, half, columns), bf16),
            pltpu.VMEM((others, chunks, halves, half, columns), bf16),
            pltpu.VMEM((others, chunks, halves, half, columns), bf16),
            dma((2,)),
            dma((n,)),
            dma((chunks,)),
            dma((n, seqs)),
            dma((n, seqs)),
            dma((chunks,)),
            dma((chunks,)),
            dma((early,)),
            dma((early,)),
            dma((others, chunks, halves)),
            dma((others, chunks, halves)),
        ],
        compiler_params=pltpu.CompilerParams(
            collective_id=0, has_side_effects=True, vmem_limit_bytes=56 * 1024 * 1024
        ),
    )(lengths, queries, kv_cache, residual, out_weight)
    normed = scaled * norm_gain.astype(f32)
    return summed.astype(bf16), normed.astype(bf16)


def solution(mesh):
    return jax.shard_map(
        functools.partial(on_device, mesh.shape["tp"]),
        mesh=mesh,
        in_specs=(
            P(("dp", "tp"), None, None),
            P(("dp", "tp"), None, None, None),
            P(("dp", "tp")),
            P(("dp", "tp"), None, None),
            P("tp", None),
            P(),
        ),
        out_specs=(P(("dp", "tp"), None, None), P(("dp", "tp"), None, None)),
        check_vma=False,
    )
```
